32 devices in a mesh: freq: 4 (over y, x), space: 8 (over z, core).
Axes of the slice: x: 2, y: 2, z: 4, core: 2. Of those that a mesh axis runs over, the one named last changes fastest.
Arguments:
- spectra: bfloat16 [2, 256, 24, 32768], P(None, 'freq', None, 'space'), may hold values from -6 to 6
- eigvecs: bfloat16 [2, 256, 4, 32768], P(None, 'freq', None, 'space'), may hold values from -6 to 6
- weights: bfloat16 [32768], P('space'), may hold values from 0.19921875 to 5
Outputs:
- filtered: float32 [3200, 32768], P(None, ('space', 'freq'))
The draws below stay inside these ranges and needn't reach their ends.
All inputs are finite; a program needn't handle non-finite values.
Results may differ from the reference program's by a relative error of at most 0.004.
Values may be sent and summed in bfloat16 or wider, within the bound.
A program may use at most 128 MiB of HBM per device.

```python
import math
import jax
import jax.numpy as jnp
from jax import lax

NFREQ = 256
MODES = 4
BLOCKS = 24
P_DEV = 4096
POINTS = 32768
TIME = 3200
N_SPACE = 8


def level_of(rng, shape, split, smallest, top_value):
    factor_of, own = 1.0, jax.random.fold_in(rng, 6)
    for position, parts in split:
        heights = jnp.exp(jax.random.uniform(jax.random.fold_in(own, position), (parts,), jnp.float32, smallest / len(split), top_value / len(split)))
        factor_of = factor_of * jnp.repeat(heights, shape[position] // parts).reshape([-1 if axis == position else 1 for axis in range(len(shape))])
    return factor_of


def gaussian(rng, extent, deviation, limit, split=(), kind=jnp.bfloat16):
    drawn = deviation * jax.random.normal(rng, extent, jnp.float32)
    if split:
        drawn = drawn * level_of(rng, extent, split, -0.22, 0.18)
    return jnp.clip(drawn, -limit, limit).astype(kind)


def setup_inputs(seed: int = 0) -> dict:
    splits = jax.random.split(jax.random.key(seed), 4)
    spectra = gaussian(splits[0], (2, NFREQ, BLOCKS, POINTS), 1.0, 6.0, ((1, 4), (3, 8)))
    eigvecs = gaussian(splits[1], (2, NFREQ, MODES, POINTS), 1.0, 6.0, ((1, 4), (3, 8)))
    weights = jnp.clip(jnp.exp(math.log(5.0) - 3.2227897 * jax.random.uniform(splits[2], (POINTS,), jnp.float32) ** level_of(splits[2], (POINTS,), ((0, 8),), -0.2, 0.2)), 0.19921875, 5.0).astype(jnp.bfloat16)
    return dict(spectra=spectra, eigvecs=eigvecs, weights=weights)


def coefficient_terms(spectra_block, weighted_block):
    spectra_real = spectra_block[0].astype(jnp.float32)
    spectra_imag = spectra_block[1].astype(jnp.float32)
    modes_real = weighted_block[0].astype(jnp.float32)
    modes_imag = weighted_block[1].astype(jnp.float32)
    highest = lax.Precision.HIGHEST
    real_terms = jnp.einsum('kmp,kbp->kbm', modes_real, spectra_real, precision=highest) + jnp.einsum('kmp,kbp->kbm', modes_imag, spectra_imag, precision=highest)
    imag_terms = jnp.einsum('kmp,kbp->kbm', modes_real, spectra_imag, precision=highest) - jnp.einsum('kmp,kbp->kbm', modes_imag, spectra_real, precision=highest)
    return jnp.stack([real_terms, imag_terms])

def rebuild(modes_block, coefficients):
    highest = lax.Precision.HIGHEST
    modes_real = modes_block[0].astype(jnp.float32)
    modes_imag = modes_block[1].astype(jnp.float32)
    coef_real = coefficients[0]
    coef_imag = coefficients[1]
    real_part = jnp.einsum('kmp,kbm->kbp', modes_real, coef_real, precision=highest) - jnp.einsum('kmp,kbm->kbp', modes_imag, coef_imag, precision=highest)
    imag_part = jnp.einsum('kmp,kbm->kbp', modes_real, coef_imag, precision=highest) + jnp.einsum('kmp,kbm->kbp', modes_imag, coef_real, precision=highest)
    return jnp.stack([real_part, imag_part]).astype(jnp.bfloat16)

def correlation_add(series):
    length = series.shape[0]
    half_length = length // 2
    window = jnp.sin(math.pi * (jnp.arange(length, dtype=jnp.float32) + 0.5) / length)
    shaped = (series * window[:, None, None]).reshape(2, half_length, series.shape[1], series.shape[2])
    zeros_block = jnp.zeros((half_length, 1, series.shape[2]), jnp.float32)
    leading = jnp.concatenate([shaped[0], zeros_block], axis=1)
    trailing = jnp.concatenate([zeros_block, shaped[1]], axis=1)
    summed = leading + trailing
    return jnp.transpose(summed, (1, 0, 2)).reshape(-1, series.shape[2])

def reference(spectra, eigvecs, weights):
    weighted = (eigvecs.astype(jnp.float32) * weights.astype(jnp.float32)).astype(jnp.bfloat16)
    factor = 1.0 / math.sqrt(POINTS)

    def partial_sum(index):
        start = (index * P_DEV).astype(jnp.int32)
        return coefficient_terms(lax.dynamic_slice_in_dim(spectra, start, P_DEV, 3), lax.dynamic_slice_in_dim(weighted, start, P_DEV, 3))
    indices = jnp.arange(N_SPACE, dtype=jnp.int32)
    coefficients = lax.optimization_barrier(jnp.sum(lax.map(partial_sum, indices), axis=0)) * factor

    def filtered_block(index):
        start = (index * P_DEV).astype(jnp.int32)
        rebuilt = rebuild(lax.dynamic_slice_in_dim(eigvecs, start, P_DEV, 3), coefficients).astype(jnp.float32)
        series = jnp.fft.ifft(rebuilt[0] + 1j * rebuilt[1], axis=0).real * math.sqrt(NFREQ)
        return correlation_add(series)
    pieces = lax.map(filtered_block, indices)
    return jnp.transpose(pieces, (1, 0, 2)).reshape(TIME, POINTS)
```

```python
import functools
import math

import jax
import jax.numpy as jnp
import numpy as np
from jax import lax
from jax.experimental import pallas as pl
from jax.experimental.pallas import tpu as pltpu
from jax.sharding import PartitionSpec as P

MESH = pl.DeviceIdType.MESH
PAIR = 16


def wait_all(copies):
    for copy in copies:
        copy.wait()


def lines_of(coefs, groups):
    real, imag = coefs
    blocks, wide = real.shape
    block = wide // (2 * groups)
    span = 2 * block
    modes = block // PAIR
    lane = lax.broadcasted_iota(jnp.int32, (blocks, span), 1)
    whole = lax.broadcasted_iota(jnp.int32, (blocks, wide), 1)

    def partners(x):
        moved = pltpu.roll(x, wide - modes, 1)
        middle = pltpu.roll(x, wide // 2 - modes, 1)
        return jnp.where(whole >= wide - modes, middle, moved)

    mates = [partners(real), partners(imag)]
    low = lane < block
    out = []
    for g in range(groups):
        own = g // 2 * span
        mate = (2 * groups - 1 - g) // 2 * span
        d = [x[:, own : own + span] for x in (real, imag)]
        p = [x[:, mate : mate + span] for x in mates]
        if g % 2:
            d = [pltpu.roll(x, block, 1) for x in d]
            p = [pltpu.roll(x, block, 1) for x in p]
        first = lane < modes
        last = lane >= span - modes
        re0, re1 = jnp.where(low, d[0], p[0]), jnp.where(low, -d[1], -p[1])
        im0, im1 = jnp.where(low, d[1], -p[1]), jnp.where(low, d[0], -p[0])
        if g == 0:
            im0 = jnp.where(first, 0.0, jnp.where(last, re0, im0))
            im1 = jnp.where(first, 0.0, jnp.where(last, re1, im1))
            re0 = jnp.where(last, 0.0, re0)
            re1 = jnp.where(last, 0.0, re1)
        out.append((jnp.concatenate([re0, re1], axis=1), jnp.concatenate([im0, im1], axis=1)))
    return out


def spread_mask(depth, modes):
    span = depth // 2
    lane = lax.broadcasted_iota(jnp.int32, (PAIR, depth), 1) % span
    kept = jnp.where(lane < span // 2, lane // modes, (span - 1 - lane) // modes)
    return kept == lax.broadcasted_iota(jnp.int32, (PAIR, depth), 0)


def stack_modes(ref, chunk, g, length):
    pieces = []
    for c in range(2):
        for start in (PAIR * g, length + 1 - PAIR * (g + 1)):
            block = ref[chunk, c, pl.ds(start, PAIR)]
            pieces.append(block.reshape(PAIR * block.shape[1], block.shape[2]))
    return jnp.concatenate(pieces, axis=0)


def rebuild(left, modes, mid_ref, g):
    rebuilt = jnp.dot(left, modes, preferred_element_type=jnp.float32).astype(jnp.bfloat16)
    for b in range(mid_ref.shape[0]):
        mid_ref[b, pl.ds(g * 2 * PAIR, 2 * PAIR)] = rebuilt[b * 2 * PAIR : (b + 1) * 2 * PAIR]


def gather_kernel(
    n_freq, n_space, group, parts, factor, early,
    spectra_ref, eigvecs_ref, weights_ref, basis_hbm, *refs,
):
    early_ref = refs[0] if early else None
    (
        late_ref, left_ref, taken, sbuf, ebuf, wbuf, wide, acc, pieces, land, own, quad, every,
        line_ref, mid_ref, carry_ref, basis_ref,
        send_a, recv_a, local_sem, s_sem, e_sem, w_sem, send_1, recv_1, send_2, recv_2, send_3, recv_3,
    ) = refs[1 if early else 0 :]
    f = lax.axis_index("freq")
    s = lax.axis_index("space")
    _, count, modes, points = eigvecs_ref.shape
    chunks, _, length1, _, tile = taken.shape
    length = length1 - 1
    width = points // n_freq
    blocks = acc.shape[1]
    half = group * modes
    halves = count // group
    groups = length // (2 * PAIR)
    cut = points // parts
    steps = halves * parts

    barrier = pltpu.get_barrier_semaphore()
    for df in range(1, n_freq):
        pl.semaphore_signal(barrier, inc=1, device_id=(lax.rem(f + df, n_freq), s), device_id_type=MESH)
    for ds in range(1, n_space):
        pl.semaphore_signal(barrier, inc=1, device_id=(f, lax.rem(s + ds, n_space)), device_id_type=MESH)

    def fetch(step, slot):
        h, i = step // parts, step % parts
        column = pl.multiple_of(i * cut, cut)
        return [
            pltpu.make_async_copy(
                spectra_ref.at[:, pl.ds(pl.multiple_of(h * (group * blocks), group * blocks), group * blocks), pl.ds(column, cut)],
                sbuf.at[slot], s_sem.at[slot],
            ),
            pltpu.make_async_copy(
                eigvecs_ref.at[:, pl.ds(h * group, group), :, pl.ds(column, cut)], ebuf.at[slot], e_sem.at[slot]
            ),
        ]

    for copy in fetch(0, 0):
        copy.start()
    small = [
        pltpu.make_async_copy(weights_ref, wbuf, w_sem.at[0]),
        pltpu.make_async_copy(basis_hbm, basis_ref, w_sem.at[1]),
    ]
    for copy in small:
        copy.start()

    def swap(j, c, df):
        target = lax.rem(f + df, n_freq)
        column = pl.multiple_of(target * width + j * tile, tile)
        return pltpu.make_async_remote_copy(
            src_ref=eigvecs_ref.at[c, :, :, pl.ds(column, tile)],
            dst_ref=taken.at[j, c, pl.ds(f * count, count)],
            send_sem=send_a.at[j, c, df], recv_sem=recv_a.at[j, c, df],
            device_id=(target, s), device_id_type=MESH,
        )

    def keep(j, c):
        column = pl.multiple_of(f * width + j * tile, tile)
        return pltpu.make_async_copy(
            eigvecs_ref.at[c, :, :, pl.ds(column, tile)], taken.at[j, c, pl.ds(f * count, count)], local_sem.at[j, c]
        )

    order = [(j, c) for j in range(chunks) for c in range(2)]
    ahead = len(order) // 2
    pl.semaphore_wait(barrier, n_freq + n_space - 2)
    for j, c in order[:ahead]:
        for df in range(1, n_freq):
            swap(j, c, df).start()
    for j, c in order:
        keep(j, c).start()

    wait_all(small)
    for i in range(parts):
        wide[i] = wbuf[i * cut : (i + 1) * cut].astype(jnp.float32).reshape(1, cut)
    acc[...] = jnp.zeros_like(acc)
    owner = lax.broadcasted_iota(jnp.int32, (blocks, 2 * half), 1) % half // modes

    def project(step, carry):
        slot = lax.rem(step, 2)

        @pl.when(step + 1 < steps)
        def _():
            for copy in fetch(step + 1, lax.rem(step + 1, 2)):
                copy.start()

        wait_all(fetch(step, slot))
        h, i = step // parts, step % parts
        weights = wide[i]
        weighted = jnp.concatenate(
            [
                (ebuf[slot, c].reshape(half, cut).astype(jnp.float32) * weights).astype(jnp.bfloat16)
                for c in range(2)
            ],
            axis=0,
        )
        for c in range(2):
            product = lax.dot_general(
                sbuf[slot, c], weighted, (((1,), (1,)), ((), ())), preferred_element_type=jnp.float32
            )
            total = acc[2 * h + c]
            for j in range(group):
                total += jnp.where(owner == j, product[j * blocks : (j + 1) * blocks], 0.0)
            acc[2 * h + c] = total
        return carry

    lax.fori_loop(0, steps, project, 0)

    rows = pieces.shape[1]
    split = blocks // rows
    for h in range(halves):
        a, b = acc[2 * h], acc[2 * h + 1]
        both = (a[:, :half] + b[:, half:], b[:, :half] - a[:, half:])
        for c in range(2):
            for q in range(split):
                pieces[(2 * h + c) * split + q] = both[c][q * rows : (q + 1) * rows]

    first = []
    for ds in range(1, n_space):
        target = lax.rem(s + ds, n_space)
        first.append(
            pltpu.make_async_remote_copy(
                src_ref=pieces.at[target], dst_ref=land.at[ds], send_sem=send_1.at[ds], recv_sem=recv_1.at[ds],
                device_id=(f, target), device_id_type=MESH,
            )
        )
        first[-1].start()
    total = pieces[s]
    for ds in range(1, n_space):
        first[ds - 1].wait_recv()
        total += land[ds]
    own[...] = total
    second = []
    for df in range(1, n_freq):
        second.append(
            pltpu.make_async_remote_copy(
                src_ref=own, dst_ref=quad.at[f], send_sem=send_2.at[df], recv_sem=recv_2.at[df],
                device_id=(lax.rem(f + df, n_freq), s), device_id_type=MESH,
            )
        )
        second[-1].start()
    for j, c in order[ahead:]:
        for df in range(1, n_freq):
            swap(j, c, df).start()
    quad[f] = total
    for copy in second:
        copy.wait_recv()
    third = []
    for ds in range(1, n_space):
        third.append(
            pltpu.make_async_remote_copy(
                src_ref=quad, dst_ref=every.at[s], send_sem=send_3.at[ds], recv_sem=recv_3.at[ds],
                device_id=(f, lax.rem(s + ds, n_space)), device_id_type=MESH,
            )
        )
        third[-1].start()
    every[s] = quad[...]
    for copy in third:
        copy.wait_recv()

    coefs = []
    for c in range(2):
        lanes = []
        for g in range(n_freq):
            for h in range(halves):
                base = (2 * h + c) * split
                lanes.append(jnp.concatenate([every[base + q, g] for q in range(split)], axis=0))
        coefs.append(jnp.concatenate(lanes, axis=1) * factor)
    for g, pair in enumerate(lines_of(coefs, groups)):
        for c in range(2):
            line_ref[g, c] = pair[c]
    mask = spread_mask(left_ref.shape[2], modes)

    def fill(g, carry):
        for c in range(2):
            lines = line_ref[g, c]
            for b in range(blocks):
                left_ref[g, (2 * b + c) * PAIR : (2 * b + c + 1) * PAIR] = jnp.where(
                    mask, lines[b : b + 1], 0.0
                ).astype(jnp.bfloat16)
        return carry

    lax.fori_loop(0, groups, fill, 0)

    def arrived(j):
        for c in range(2):
            keep(j, c).wait()
            for df in range(1, n_freq):
                swap(j, c, df).wait_recv()
        for c in range(2):
            taken[j, c, length] = taken[j, c, length // 2]

    half_length = length // 2

    def finish(j, carry):
        arrived(j)

        def one(g, inner):
            rebuild(left_ref[g], stack_modes(taken, j, g, length), mid_ref, g)
            return inner

        lax.fori_loop(0, groups, one, 0)
        carry_ref[...] = jnp.zeros_like(carry_ref)

        def add(b, inner):
            series = jnp.dot(basis_ref[...], mid_ref[b], preferred_element_type=jnp.float32)
            early_ref[j, pl.ds(pl.multiple_of(b * half_length, half_length), half_length)] = (
                series[:half_length] + carry_ref[...]
            )
            carry_ref[...] = series[half_length:]
            return inner

        lax.fori_loop(0, blocks, add, 0)
        early_ref[j, blocks * half_length :] = carry_ref[...]
        return carry

    if early:
        lax.fori_loop(0, early, finish, 0)
    for j in range(early, chunks):
        arrived(j)

        def arrange(g, carry):
            late_ref[j - early, g] = stack_modes(taken, j, g, length)
            return carry

        lax.fori_loop(0, groups, arrange, 0)
    for copy in first + second + third:
        copy.wait_send()
    for j, c in order:
        for df in range(1, n_freq):
            swap(j, c, df).wait_send()


def gather(spectra, eigvecs, weights, basis, n_freq, n_space, blocks, factor, tile, early):
    _, count, modes, points = eigvecs.shape
    length = n_freq * count
    group = min(2 * PAIR, count)
    half = group * modes
    halves = count // group
    width = points // n_freq
    chunks = width // tile
    parts = 4
    cut = points // parts
    groups = length // (2 * PAIR)
    depth = 4 * PAIR * modes
    rows = halves * 2 * blocks // n_space
    out_rows = (blocks + 1) * (length // 2)
    hbm = pl.BlockSpec(memory_space=pltpu.HBM)
    vmem = pl.BlockSpec(memory_space=pltpu.VMEM)
    out_shape = [
        jax.ShapeDtypeStruct((chunks - early, groups, depth, tile), jnp.bfloat16),
        jax.ShapeDtypeStruct((groups, blocks * 2 * PAIR, depth), jnp.bfloat16),
    ]
    if early:
        out_shape = [jax.ShapeDtypeStruct((early, out_rows, tile), jnp.float32)] + out_shape
    dma = pltpu.SemaphoreType.DMA
    return pl.pallas_call(
        functools.partial(gather_kernel, n_freq, n_space, group, parts, factor, early),
        out_shape=out_shape,
        in_specs=[hbm] * 4,
        out_specs=[vmem] * len(out_shape),
        scratch_shapes=[
            pltpu.VMEM((chunks, 2, length + 1, modes, tile), jnp.bfloat16),
            pltpu.VMEM((2, 2, group * blocks, cut), jnp.bfloat16),
            pltpu.VMEM((2, 2, group, modes, cut), jnp.bfloat16),
            pltpu.VMEM((points,), jnp.bfloat16),
            pltpu.VMEM((parts, 1, cut), jnp.float32),
            pltpu.VMEM((2 * halves, blocks, 2 * half), jnp.float32),
            pltpu.VMEM((n_space, rows, half), jnp.float32),
            pltpu.VMEM((n_space, rows, half), jnp.float32),
            pltpu.VMEM((rows, half), jnp.float32),
            pltpu.VMEM((n_freq, rows, half), jnp.float32),
            pltpu.VMEM((n_space, n_freq, rows, half), jnp.float32),
            pltpu.VMEM((groups, 2, blocks, depth), jnp.float32),
            pltpu.VMEM((blocks, length, tile), jnp.bfloat16),
            pltpu.VMEM((length // 2, tile), jnp.float32),
            pltpu.VMEM((length, length), jnp.bfloat16),
            dma((chunks, 2, n_freq)),
            dma((chunks, 2, n_freq)),
            dma((chunks, 2)),
            dma((2,)),
            dma((2,)),
            dma((2,)),
            dma((n_space,)),
            dma((n_space,)),
            dma((n_freq,)),
            dma((n_freq,)),
            dma((n_space,)),
            dma((n_space,)),
        ],
        compiler_params=pltpu.CompilerParams(
            collective_id=0, has_side_effects=True, vmem_limit_bytes=32 << 20
        ),
        cost_estimate=pl.CostEstimate(
            flops=8 * spectra.shape[1] * points * 2 * half, bytes_accessed=4 * spectra.size, transcendentals=0
        ),
        name="gather",
    )(*[pltpu.with_memory_space_constraint(x, pltpu.HBM) for x in (spectra, eigvecs, weights, basis)])


def finish_kernel(early, tile, *refs):
    if early:
        early_ref, refs = refs[0], refs[1:]
    late_ref, left_ref, basis_ref, out_ref, mid_ref, result, copy_sem, late_sem = refs
    blocks, length, _ = mid_ref.shape
    groups = left_ref.shape[0]
    half_length = length // 2
    runs = late_sem.shape[1]
    copies = []
    for j in range(early):
        copies.append(
            pltpu.make_async_copy(early_ref.at[j], out_ref.at[:, j * tile : (j + 1) * tile], copy_sem.at[j])
        )
        copies[-1].start()
    for l in range(late_ref.shape[0]):
        for g in range(groups):
            rebuild(left_ref[g], late_ref[l, g], mid_ref, g)
        carry = None
        done = 0
        for b in range(blocks):
            series = jnp.dot(basis_ref[...], mid_ref[b], preferred_element_type=jnp.float32)
            lead = series[:half_length]
            result[l, b * half_length : (b + 1) * half_length] = lead if carry is None else lead + carry
            carry = series[half_length:]
            last = b == blocks - 1
            if last:
                result[l, blocks * half_length :] = carry
            if last or (b + 1) % (blocks // runs) == 0:
                stop = (b + 1 + last) * half_length
                column = (early + l) * tile
                copies.append(
                    pltpu.make_async_copy(
                        result.at[l, done:stop], out_ref.at[done:stop, column : column + tile],
                        late_sem.at[l, (b + 1) // (blocks // runs) - 1],
                    )
                )
                copies[-1].start()
                done = stop
    wait_all(copies)


def finish(arrays, basis, blocks, length, width, tile, early):
    late, left = arrays[-2:]
    out_rows = (blocks + 1) * (length // 2)
    vmem = pl.BlockSpec(memory_space=pltpu.VMEM)
    runs = 4
    return pl.pallas_call(
        functools.partial(finish_kernel, early, tile),
        out_shape=jax.ShapeDtypeStruct((out_rows, width), jnp.float32),
        in_specs=[vmem] * (len(arrays) + 1),
        out_specs=pl.BlockSpec(memory_space=pltpu.HBM),
        scratch_shapes=[
            pltpu.VMEM((blocks, length, tile), jnp.bfloat16),
            pltpu.VMEM((late.shape[0], out_rows, tile), jnp.float32),
            pltpu.SemaphoreType.DMA((max(early, 1),)),
            pltpu.SemaphoreType.DMA((late.shape[0], runs)),
        ],
        compiler_params=pltpu.CompilerParams(vmem_limit_bytes=24 << 20),
        cost_estimate=pl.CostEstimate(
            flops=4 * length * length * blocks * tile, bytes_accessed=4 * out_rows * width, transcendentals=0
        ),
        name="finish",
    )(*arrays, basis)


def basis_of(length):
    groups = length // (2 * PAIR)
    freq = np.arange(length // 2).reshape(groups, 1, PAIR)
    time = np.arange(length).reshape(length, 1, 1, 1)
    phase = 2.0 * np.pi * ((freq * time) % length) / length
    both = np.concatenate([np.cos(phase), -np.sin(phase)], axis=2)
    both[:, 0, 1, 0] = 1.0 - 2.0 * (np.arange(length) % 2)
    window = np.sin(np.pi * (np.arange(length) + 0.5) / length) / math.sqrt(length)
    return jnp.asarray((both.reshape(length, length) * window[:, None]).astype(np.float32)).astype(jnp.bfloat16)


def body(spectra, eigvecs, weights):
    n_freq = lax.axis_size("freq")
    n_space = lax.axis_size("space")
    _, count, blocks, points = spectra.shape
    factor = 1.0 / math.sqrt(points * n_space)
    length = n_freq * count
    width = points // n_freq
    tile = 256 if width % 256 == 0 else width
    early = width // tile - 1
    basis = basis_of(length)
    spectra = spectra.reshape(2, count * blocks, points)
    arrays = gather(spectra, eigvecs, weights, basis, n_freq, n_space, blocks, factor, tile, early)
    return finish(arrays, basis, blocks, length, width, tile, early)


def solution(mesh):
    placed = (P(None, "freq", None, "space"), P(None, "freq", None, "space"), P("space"))
    return jax.shard_map(
        body, mesh=mesh, in_specs=placed, out_specs=P(None, ("space", "freq")), check_vma=False
    )
```

```python
import functools
import math

import jax
import jax.numpy as jnp
import numpy as np
from jax import lax
from jax.experimental import pallas as pl
from jax.experimental.pallas import tpu as pltpu
from jax.sharding import PartitionSpec as P

MESH = pl.DeviceIdType.MESH
PAIR = 16


def wait_all(copies):
    for copy in copies:
        copy.wait()


def lines_of(coefs, groups):
    real, imag = coefs
    blocks, wide = real.shape
    block = wide // (2 * groups)
    span = 2 * block
    modes = block // PAIR
    lane = lax.broadcasted_iota(jnp.int32, (blocks, span), 1)
    whole = lax.broadcasted_iota(jnp.int32, (blocks, wide), 1)

    def partners(x):
        moved = pltpu.roll(x, wide - modes, 1)
        middle = pltpu.roll(x, wide // 2 - modes, 1)
        return jnp.where(whole >= wide - modes, middle, moved)

    mates = [partners(real), partners(imag)]
    low = lane < block
    out = []
    for g in range(groups):
        own = g // 2 * span
        mate = (2 * groups - 1 - g) // 2 * span
        d = [x[:, own : own + span] for x in (real, imag)]
        p = [x[:, mate : mate + span] for x in mates]
        if g % 2:
            d = [pltpu.roll(x, block, 1) for x in d]
            p = [pltpu.roll(x, block, 1) for x in p]
        first = lane < modes
        last = lane >= span - modes
        re0, re1 = jnp.where(low, d[0], p[0]), jnp.where(low, -d[1], -p[1])
        im0, im1 = jnp.where(low, d[1], -p[1]), jnp.where(low, d[0], -p[0])
        if g == 0:
            im0 = jnp.where(first, 0.0, jnp.where(last, re0, im0))
            im1 = jnp.where(first, 0.0, jnp.where(last, re1, im1))
            re0 = jnp.where(last, 0.0, re0)
            re1 = jnp.where(last, 0.0, re1)
        out.append((jnp.concatenate([re0, re1], axis=1), jnp.concatenate([im0, im1], axis=1)))
    return out


def spread_mask(depth, modes):
    span = depth // 2
    lane = lax.broadcasted_iota(jnp.int32, (PAIR, depth), 1) % span
    kept = jnp.where(lane < span // 2, lane // modes, (span - 1 - lane) // modes)
    return kept == lax.broadcasted_iota(jnp.int32, (PAIR, depth), 0)


def stack_modes(ref, tiles, g, length):
    pieces = []
    for c in range(2):
        for start in (PAIR * g, length + 1 - PAIR * (g + 1)):
            blocks = [ref[tile, c, pl.ds(start, PAIR)] for tile in tiles]
            blocks = [block.reshape(PAIR * block.shape[1], block.shape[2]) for block in blocks]
            pieces.append(blocks[0] if len(blocks) == 1 else jnp.concatenate(blocks, axis=1))
    return jnp.concatenate(pieces, axis=0)


def synthesize(modes_of, left_ref, basis_ref, mid_ref, wide, put):
    blocks, length, _ = mid_ref.shape
    half_length = length // 2
    for g in range(left_ref.shape[0]):
        rebuilt = jnp.dot(left_ref[g], modes_of(g), preferred_element_type=jnp.float32).astype(jnp.bfloat16)
        for b in range(blocks):
            mid_ref[b, g * 2 * PAIR : (g + 1) * 2 * PAIR, :wide] = rebuilt[b * 2 * PAIR : (b + 1) * 2 * PAIR]
    tail = None
    for b in range(blocks):
        series = jnp.dot(basis_ref[...], mid_ref[b, :, :wide], preferred_element_type=jnp.float32)
        lead = series[:half_length]
        put(b, lead if tail is None else lead + tail)
        tail = series[half_length:]
    put(blocks, tail)


def gather_kernel(
    n_freq, n_space, group, parts, factor,
    spectra_ref, eigvecs_ref, weights_ref, basis_hbm, *refs,
):
    (
        early_ref, late_ref, left_ref, taken, sbuf, ebuf, wbuf, wide, acc, pieces, land, own, every,
        line_ref, mid_ref, basis_ref,
        send_a, recv_a, local_sem, s_sem, e_sem, w_sem, send_1, recv_1, send_2, recv_2, send_3, recv_3,
    ) = refs
    f = lax.axis_index("freq")
    s = lax.axis_index("space")
    _, count, modes, points = eigvecs_ref.shape
    chunks, _, length1, _, tile = taken.shape
    length = length1 - 1
    width = points // n_freq
    blocks = acc.shape[1]
    half = group * modes
    halves = count // group
    groups = length // (2 * PAIR)
    cut = points // parts
    steps = halves * parts

    barrier = pltpu.get_barrier_semaphore()
    for df in range(1, n_freq):
        pl.semaphore_signal(barrier, inc=1, device_id=(lax.rem(f + df, n_freq), s), device_id_type=MESH)
    bits = [1 << i for i in range(n_space.bit_length() - 1)]
    mates = [s + bit - 2 * bit * (s // bit % 2) for bit in bits]
    for mate in mates:
        pl.semaphore_signal(barrier, inc=1, device_id=(f, mate), device_id_type=MESH)

    def fetch(step, slot):
        h, i = step // parts, step % parts
        column = pl.multiple_of(i * cut, cut)
        return [
            pltpu.make_async_copy(
                spectra_ref.at[:, pl.ds(pl.multiple_of(h * (group * blocks), group * blocks), group * blocks), pl.ds(column, cut)],
                sbuf.at[slot], s_sem.at[slot],
            ),
            pltpu.make_async_copy(
                eigvecs_ref.at[:, pl.ds(h * group, group), :, pl.ds(column, cut)], ebuf.at[slot], e_sem.at[slot]
            ),
        ]

    for copy in fetch(0, 0):
        copy.start()
    small = [
        pltpu.make_async_copy(weights_ref, wbuf, w_sem.at[0]),
        pltpu.make_async_copy(basis_hbm, basis_ref, w_sem.at[1]),
    ]
    for copy in small:
        copy.start()

    def swap(j, c, df):
        target = lax.rem(f + df, n_freq)
        column = pl.multiple_of(target * width + j * tile, tile)
        return pltpu.make_async_remote_copy(
            src_ref=eigvecs_ref.at[c, :, :, pl.ds(column, tile)],
            dst_ref=taken.at[j, c, pl.ds(f * count, count)],
            send_sem=send_a.at[j, c, df], recv_sem=recv_a.at[j, c, df],
            device_id=(target, s), device_id_type=MESH,
        )

    def keep(j, c):
        column = pl.multiple_of(f * width + j * tile, tile)
        return pltpu.make_async_copy(
            eigvecs_ref.at[c, :, :, pl.ds(column, tile)], taken.at[j, c, pl.ds(f * count, count)], local_sem.at[j, c]
        )

    order = [(j, c) for j in range(chunks) for c in range(2)]
    ahead = len(order) // 2
    pl.semaphore_wait(barrier, n_freq - 1 + len(bits))
    for j, c in order[:ahead]:
        for df in range(1, n_freq):
            swap(j, c, df).start()
    for j, c in order:
        keep(j, c).start()

    wait_all(small)
    for i in range(parts):
        wide[i] = wbuf[i * cut : (i + 1) * cut].astype(jnp.float32).reshape(1, cut)
    acc[...] = jnp.zeros_like(acc)
    owner = lax.broadcasted_iota(jnp.int32, (blocks, 2 * half), 1) % half // modes

    def project(step, carry):
        slot = lax.rem(step, 2)

        @pl.when(step + 1 < steps)
        def _():
            for copy in fetch(step + 1, lax.rem(step + 1, 2)):
                copy.start()

        wait_all(fetch(step, slot))
        h, i = step // parts, step % parts
        weights = wide[i]
        weighted = jnp.concatenate(
            [
                (ebuf[slot, c].reshape(half, cut).astype(jnp.float32) * weights).astype(jnp.bfloat16)
                for c in range(2)
            ],
            axis=0,
        )
        for c in range(2):
            product = lax.dot_general(
                sbuf[slot, c], weighted, (((1,), (1,)), ((), ())), preferred_element_type=jnp.float32
            )
            total = acc[2 * h + c]
            for j in range(group):
                total += jnp.where(owner == j, product[j * blocks : (j + 1) * blocks], 0.0)
            acc[2 * h + c] = total
        return carry

    lax.fori_loop(0, steps, project, 0)

    rows = pieces.shape[1]
    split = blocks // rows
    for h in range(halves):
        a, b = acc[2 * h], acc[2 * h + 1]
        both = (a[:, :half] + b[:, half:], b[:, :half] - a[:, half:])
        for c in range(2):
            for q in range(split):
                pieces[(2 * h + c) * split + q] = both[c][q * rows : (q + 1) * rows]

    started = []

    def send(source, target, sems, where):
        copy = pltpu.make_async_remote_copy(
            src_ref=source, dst_ref=target, send_sem=sems[0], recv_sem=sems[1], device_id=where, device_id_type=MESH
        )
        copy.start()
        started.append(copy)
        return copy

    base, size = 0, n_space
    bases = []
    for i, (bit, mate) in enumerate(zip(bits, mates)):
        size //= 2
        mine = base + s // bit % 2 * size
        other = base + size - s // bit % 2 * size
        copy = send(
            pieces.at[pl.ds(other, size)], land.at[pl.ds(size, size)], (send_1.at[i], recv_1.at[i]), (f, mate)
        )
        copy.wait_recv()
        pieces[pl.ds(mine, size)] = pieces[pl.ds(mine, size)] + land[size : 2 * size]
        base = mine
        bases.append((base, size))
    own[...] = (pieces[base] * factor).astype(own.dtype)
    second = []
    for df in range(1, n_freq):
        second.append(
            send(own, every.at[base, f], (send_2.at[df], recv_2.at[df]), (lax.rem(f + df, n_freq), s))
        )
    for j, c in order[ahead:]:
        for df in range(1, n_freq):
            swap(j, c, df).start()
    every[base, f] = own[...]
    for copy in second:
        copy.wait_recv()
    for i, mate in reversed(list(enumerate(mates))):
        low, size = bases[i]
        block = every.at[pl.ds(low, size)]
        send(block, block, (send_3.at[i], recv_3.at[i]), (f, mate)).wait_recv()

    coefs = []
    for c in range(2):
        lanes = []
        for g in range(n_freq):
            for h in range(halves):
                base = (2 * h + c) * split
                lanes.append(
                    jnp.concatenate([every[base + q, g].astype(jnp.float32) for q in range(split)], axis=0)
                )
        coefs.append(jnp.concatenate(lanes, axis=1))
    for g, pair in enumerate(lines_of(coefs, groups)):
        for c in range(2):
            line_ref[g, c] = pair[c]
    mask = spread_mask(left_ref.shape[2], modes)

    def fill(g, carry):
        for c in range(2):
            lines = line_ref[g, c]
            for b in range(blocks):
                left_ref[g, (2 * b + c) * PAIR : (2 * b + c + 1) * PAIR] = jnp.where(
                    mask, lines[b : b + 1], 0.0
                ).astype(jnp.bfloat16)
        return carry

    lax.fori_loop(0, groups, fill, 0)

    def arrived(j):
        for c in range(2):
            keep(j, c).wait()
            for df in range(1, n_freq):
                swap(j, c, df).wait_recv()
        for c in range(2):
            taken[j, c, length] = taken[j, c, length // 2]

    half_length = length // 2

    def put_at(column, wide):
        def put(b, rows):
            early_ref[b * half_length : (b + 1) * half_length, pl.ds(column, wide)] = rows

        return put

    def finish(j, carry):
        tiles = (2 * j, 2 * j + 1)
        for one in tiles:
            arrived(one)
        synthesize(
            lambda g: stack_modes(taken, tiles, g, length), left_ref, basis_ref, mid_ref, 2 * tile,
            put_at(pl.multiple_of(j * 2 * tile, 2 * tile), 2 * tile),
        )
        return carry

    early = chunks - 1
    if early >= 2:
        lax.fori_loop(0, early // 2, finish, 0)
    if early % 2:
        arrived(early - 1)
        synthesize(
            lambda g: stack_modes(taken, (early - 1,), g, length), left_ref, basis_ref, mid_ref, tile,
            put_at((early - 1) * tile, tile),
        )
    arrived(early)

    def arrange(g, carry):
        late_ref[g] = stack_modes(taken, (early,), g, length)
        return carry

    lax.fori_loop(0, groups, arrange, 0)
    for copy in started:
        copy.wait_send()
    for j, c in order:
        for df in range(1, n_freq):
            swap(j, c, df).wait_send()


def gather(spectra, eigvecs, weights, basis, n_freq, n_space, blocks, factor, tile):
    _, count, modes, points = eigvecs.shape
    length = n_freq * count
    group = min(2 * PAIR, count)
    half = group * modes
    halves = count // group
    width = points // n_freq
    chunks = width // tile
    parts = 4
    cut = points // parts
    groups = length // (2 * PAIR)
    depth = 4 * PAIR * modes
    rows = halves * 2 * blocks // n_space
    out_rows = (blocks + 1) * (length // 2)
    hbm = pl.BlockSpec(memory_space=pltpu.HBM)
    vmem = pl.BlockSpec(memory_space=pltpu.VMEM)
    out_shape = [
        jax.ShapeDtypeStruct((out_rows, width - tile), jnp.float32),
        jax.ShapeDtypeStruct((groups, depth, tile), jnp.bfloat16),
        jax.ShapeDtypeStruct((groups, blocks * 2 * PAIR, depth), jnp.bfloat16),
    ]
    dma = pltpu.SemaphoreType.DMA
    return pl.pallas_call(
        functools.partial(gather_kernel, n_freq, n_space, group, parts, factor),
        out_shape=out_shape,
        in_specs=[hbm] * 4,
        out_specs=[vmem] * len(out_shape),
        scratch_shapes=[
            pltpu.VMEM((chunks, 2, length + 1, modes, tile), jnp.bfloat16),
            pltpu.VMEM((2, 2, group * blocks, cut), jnp.bfloat16),
            pltpu.VMEM((2, 2, group, modes, cut), jnp.bfloat16),
            pltpu.VMEM((points,), jnp.bfloat16),
            pltpu.VMEM((parts, 1, cut), jnp.float32),
            pltpu.VMEM((2 * halves, blocks, 2 * half), jnp.float32),
            pltpu.VMEM((n_space, rows, half), jnp.float32),
            pltpu.VMEM((n_space, rows, half), jnp.float32),
            pltpu.VMEM((rows, half), jnp.bfloat16),
            pltpu.VMEM((n_space, n_freq, rows, half), jnp.bfloat16),
            pltpu.VMEM((groups, 2, blocks, depth), jnp.float32),
            pltpu.VMEM((blocks, length, 2 * tile), jnp.bfloat16),
            pltpu.VMEM((length, length), jnp.bfloat16),
            dma((chunks, 2, n_freq)),
            dma((chunks, 2, n_freq)),
            dma((chunks, 2)),
            dma((2,)),
            dma((2,)),
            dma((2,)),
            dma((n_space,)),
            dma((n_space,)),
            dma((n_freq,)),
            dma((n_freq,)),
            dma((n_space,)),
            dma((n_space,)),
        ],
        compiler_params=pltpu.CompilerParams(
            collective_id=0, has_side_effects=True, vmem_limit_bytes=32 << 20
        ),
        cost_estimate=pl.CostEstimate(
            flops=8 * spectra.shape[1] * points * 2 * half, bytes_accessed=4 * spectra.size, transcendentals=0
        ),
        name="gather",
    )(*[pltpu.with_memory_space_constraint(x, pltpu.HBM) for x in (spectra, eigvecs, weights, basis)])


def finish_kernel(early_ref, late_ref, left_ref, basis_ref, out_ref, mid_ref, result, early_sem, late_sem):
    blocks, length, tile = mid_ref.shape
    half_length = length // 2
    rest = early_ref.shape[1]
    runs = late_sem.shape[0]
    copies = [pltpu.make_async_copy(early_ref, out_ref.at[:, :rest], early_sem)]
    copies[0].start()

    def put(b, rows):
        result[b * half_length : (b + 1) * half_length] = rows
        count = b + 1 if b < blocks - 1 else b
        if b != blocks - 1 and count % (blocks // runs) == 0:
            run = count // (blocks // runs) - 1
            start = run * (blocks // runs) * half_length
            span = slice(start, (b + 1) * half_length)
            copies.append(
                pltpu.make_async_copy(result.at[span], out_ref.at[span, rest : rest + tile], late_sem.at[run])
            )
            copies[-1].start()

    synthesize(lambda g: late_ref[g], left_ref, basis_ref, mid_ref, tile, put)
    wait_all(copies)


def finish(arrays, basis, blocks, length, width, tile):
    out_rows = (blocks + 1) * (length // 2)
    vmem = pl.BlockSpec(memory_space=pltpu.VMEM)
    runs = 4
    return pl.pallas_call(
        finish_kernel,
        out_shape=jax.ShapeDtypeStruct((out_rows, width), jnp.float32),
        in_specs=[vmem] * (len(arrays) + 1),
        out_specs=pl.BlockSpec(memory_space=pltpu.HBM),
        scratch_shapes=[
            pltpu.VMEM((blocks, length, tile), jnp.bfloat16),
            pltpu.VMEM((out_rows, tile), jnp.float32),
            pltpu.SemaphoreType.DMA,
            pltpu.SemaphoreType.DMA((runs,)),
        ],
        compiler_params=pltpu.CompilerParams(vmem_limit_bytes=24 << 20),
        cost_estimate=pl.CostEstimate(
            flops=4 * length * length * blocks * tile, bytes_accessed=4 * out_rows * width, transcendentals=0
        ),
        name="finish",
    )(*arrays, basis)


def basis_of(length):
    groups = length // (2 * PAIR)
    freq = np.arange(length // 2).reshape(groups, 1, PAIR)
    time = np.arange(length).reshape(length, 1, 1, 1)
    phase = 2.0 * np.pi * ((freq * time) % length) / length
    both = np.concatenate([np.cos(phase), -np.sin(phase)], axis=2)
    both[:, 0, 1, 0] = 1.0 - 2.0 * (np.arange(length) % 2)
    window = np.sin(np.pi * (np.arange(length) + 0.5) / length) / math.sqrt(length)
    return jnp.asarray((both.reshape(length, length) * window[:, None]).astype(np.float32)).astype(jnp.bfloat16)


def body(spectra, eigvecs, weights):
    n_freq = lax.axis_size("freq")
    n_space = lax.axis_size("space")
    _, count, blocks, points = spectra.shape
    factor = 1.0 / math.sqrt(points * n_space)
    length = n_freq * count
    width = points // n_freq
    tile = 128
    basis = basis_of(length)
    spectra = spectra.reshape(2, count * blocks, points)
    arrays = gather(spectra, eigvecs, weights, basis, n_freq, n_space, blocks, factor, tile)
    return finish(arrays, basis, blocks, length, width, tile)


def solution(mesh):
    placed = (P(None, "freq", None, "space"), P(None, "freq", None, "space"), P("space"))
    return jax.shard_map(
        body, mesh=mesh, in_specs=placed, out_specs=P(None, ("space", "freq")), check_vma=False
    )
```

```python
import functools
import math

import jax
import jax.numpy as jnp
import numpy as np
from jax import lax
from jax.experimental import pallas as pl
from jax.experimental.pallas import tpu as pltpu
from jax.sharding import PartitionSpec as P

MESH = pl.DeviceIdType.MESH
PAIR = 16
AHEAD = 9


def wait_all(copies):
    for copy in copies:
        copy.wait()


def lines_of(coefs, groups):
    real, imag = coefs
    blocks, wide = real.shape
    block = wide // (2 * groups)
    span = 2 * block
    modes = block // PAIR
    lane = lax.broadcasted_iota(jnp.int32, (blocks, span), 1)
    whole = lax.broadcasted_iota(jnp.int32, (blocks, wide), 1)

    def partners(x):
        moved = pltpu.roll(x, wide - modes, 1)
        middle = pltpu.roll(x, wide // 2 - modes, 1)
        return jnp.where(whole >= wide - modes, middle, moved)

    mates = [partners(real), partners(imag)]
    low = lane < block
    out = []
    for g in range(groups):
        own = g // 2 * span
        mate = (2 * groups - 1 - g) // 2 * span
        d = [x[:, own : own + span] for x in (real, imag)]
        p = [x[:, mate : mate + span] for x in mates]
        if g % 2:
            d = [pltpu.roll(x, block, 1) for x in d]
            p = [pltpu.roll(x, block, 1) for x in p]
        first = lane < modes
        last = lane >= span - modes
        re0, re1 = jnp.where(low, d[0], p[0]), jnp.where(low, -d[1], -p[1])
        im0, im1 = jnp.where(low, d[1], -p[1]), jnp.where(low, d[0], -p[0])
        if g == 0:
            im0 = jnp.where(first, 0.0, jnp.where(last, re0, im0))
            im1 = jnp.where(first, 0.0, jnp.where(last, re1, im1))
            re0 = jnp.where(last, 0.0, re0)
            re1 = jnp.where(last, 0.0, re1)
        out.append((jnp.concatenate([re0, re1], axis=1), jnp.concatenate([im0, im1], axis=1)))
    return out


def spread_mask(depth, modes):
    span = depth // 2
    lane = lax.broadcasted_iota(jnp.int32, (PAIR, depth), 1) % span
    kept = jnp.where(lane < span // 2, lane // modes, (span - 1 - lane) // modes)
    return kept == lax.broadcasted_iota(jnp.int32, (PAIR, depth), 0)


def stack_modes(ref, tile, g, length):
    pieces = []
    for c in range(2):
        for start in (PAIR * g, length + 1 - PAIR * (g + 1)):
            block = ref[tile, c, pl.ds(start, PAIR)]
            pieces.append(block.reshape(PAIR * block.shape[1], block.shape[2]))
    return jnp.concatenate(pieces, axis=0)


def synthesize(modes_of, left_ref, basis_ref, mid_ref, wide, put):
    blocks, length, _ = mid_ref.shape
    half_length = length // 2
    for g in range(left_ref.shape[0]):
        rebuilt = jnp.dot(left_ref[g], modes_of(g), preferred_element_type=jnp.float32).astype(jnp.bfloat16)
        for b in range(blocks):
            mid_ref[b, g * 2 * PAIR : (g + 1) * 2 * PAIR, :wide] = rebuilt[b * 2 * PAIR : (b + 1) * 2 * PAIR]
    tail = None
    for b in range(blocks):
        series = jnp.dot(basis_ref[...], mid_ref[b, :, :wide], preferred_element_type=jnp.float32)
        lead = series[:half_length]
        put(b, lead if tail is None else lead + tail)
        tail = series[half_length:]
    put(blocks, tail)


def gather_kernel(
    n_freq, n_space, group, parts, factor, wides,
    spectra_ref, eigvecs_ref, weights_ref, basis_hbm, *refs,
):
    (
        early_ref, late_ref, left_ref, broad, narrow, sbuf, ebuf, wbuf, wide, acc, pieces, land, below, above, upward, downward, own, every,
        line_ref, mid_ref, basis_ref,
        send_b, recv_b, send_n, recv_n, local_b, local_n, s_sem, e_sem, w_sem, send_1, recv_1, send_2, recv_2, send_3, recv_3,
    ) = refs
    f = lax.axis_index("freq")
    s = lax.axis_index("space")
    _, count, modes, points = eigvecs_ref.shape
    narrows, _, length, _, tile = narrow.shape
    length -= 1
    width = points // n_freq
    blocks = acc.shape[1]
    half = group * modes
    halves = count // group
    groups = length // (2 * PAIR)
    cut = points // parts
    steps = halves * parts

    barrier = pltpu.get_barrier_semaphore()
    for df in range(1, n_freq):
        pl.semaphore_signal(barrier, inc=1, device_id=(lax.rem(f + df, n_freq), s), device_id_type=MESH)
    z, top = s // 2, n_space // 2 - 1
    mate = s + 1 - 2 * (s % 2)
    pl.semaphore_signal(barrier, inc=1, device_id=(f, mate), device_id_type=MESH)

    @pl.when(z > 0)
    def _():
        pl.semaphore_signal(barrier, inc=1, device_id=(f, s - 2), device_id_type=MESH)

    @pl.when(z < top)
    def _():
        pl.semaphore_signal(barrier, inc=1, device_id=(f, s + 2), device_id_type=MESH)

    def fetch(step, slot):
        h, i = step // parts, step % parts
        column = pl.multiple_of(i * cut, cut)
        return [
            pltpu.make_async_copy(
                spectra_ref.at[:, pl.ds(pl.multiple_of(h * (group * blocks), group * blocks), group * blocks), pl.ds(column, cut)],
                sbuf.at[slot], s_sem.at[slot],
            ),
            pltpu.make_async_copy(
                eigvecs_ref.at[:, pl.ds(h * group, group), :, pl.ds(column, cut)], ebuf.at[slot], e_sem.at[slot]
            ),
        ]

    for copy in fetch(0, 0):
        copy.start()
    small = [
        pltpu.make_async_copy(weights_ref, wbuf, w_sem.at[0]),
        pltpu.make_async_copy(basis_hbm, basis_ref, w_sem.at[1]),
    ]
    for copy in small:
        copy.start()

    part = count // 2

    def swap_broad(j, c, r, df):
        target = lax.rem(f + df, n_freq)
        column = pl.multiple_of(target * width + j * 2 * tile, 2 * tile)
        return pltpu.make_async_remote_copy(
            src_ref=eigvecs_ref.at[c, r * part : (r + 1) * part, :, pl.ds(column, 2 * tile)],
            dst_ref=broad.at[j, c, pl.ds(f * count + r * part, part)],
            send_sem=send_b.at[j, c, r, df], recv_sem=recv_b.at[j, c, r, df],
            device_id=(target, s), device_id_type=MESH,
        )

    def swap_narrow(j, c, df):
        target = lax.rem(f + df, n_freq)
        column = pl.multiple_of(target * width + (2 * wides + j) * tile, tile)
        return pltpu.make_async_remote_copy(
            src_ref=eigvecs_ref.at[c, :, :, pl.ds(column, tile)],
            dst_ref=narrow.at[j, c, pl.ds(f * count, count)],
            send_sem=send_n.at[j, c, df], recv_sem=recv_n.at[j, c, df],
            device_id=(target, s), device_id_type=MESH,
        )

    def keep_broad(j, c):
        column = pl.multiple_of(f * width + j * 2 * tile, 2 * tile)
        return pltpu.make_async_copy(
            eigvecs_ref.at[c, :, :, pl.ds(column, 2 * tile)], broad.at[j, c, pl.ds(f * count, count)], local_b.at[j, c]
        )

    def keep_narrow(j, c):
        column = pl.multiple_of(f * width + (2 * wides + j) * tile, tile)
        return pltpu.make_async_copy(
            eigvecs_ref.at[c, :, :, pl.ds(column, tile)], narrow.at[j, c, pl.ds(f * count, count)], local_n.at[j, c]
        )

    order = [
        functools.partial(swap_broad, j, c, r) for j in range(wides) for c in range(2) for r in range(2)
    ] + [functools.partial(swap_narrow, j, c) for j in range(narrows) for c in range(2)]
    ahead = AHEAD * len(order) // 16
    lower, upper = (z + top) // (top + 1), (2 * top - z) // (top + 1)
    pl.semaphore_wait(barrier, n_freq + lower + upper)
    for swap in order[:ahead]:
        for df in range(1, n_freq):
            swap(df).start()
    for c in range(2):
        for j in range(wides):
            keep_broad(j, c).start()
        for j in range(narrows):
            keep_narrow(j, c).start()

    wait_all(small)
    for i in range(parts):
        wide[i] = wbuf[i * cut : (i + 1) * cut].astype(jnp.float32).reshape(1, cut)
    acc[...] = jnp.zeros_like(acc)
    owner = lax.broadcasted_iota(jnp.int32, (blocks, 2 * half), 1) % half // modes

    def project(step, carry):
        slot = lax.rem(step, 2)

        @pl.when(step + 1 < steps)
        def _():
            for copy in fetch(step + 1, lax.rem(step + 1, 2)):
                copy.start()

        wait_all(fetch(step, slot))
        h, i = step // parts, step % parts
        weights = wide[i]
        weighted = jnp.concatenate(
            [
                (ebuf[slot, c].reshape(half, cut).astype(jnp.float32) * weights).astype(jnp.bfloat16)
                for c in range(2)
            ],
            axis=0,
        )
        for c in range(2):
            product = lax.dot_general(
                sbuf[slot, c], weighted, (((1,), (1,)), ((), ())), preferred_element_type=jnp.float32
            )
            total = acc[2 * h + c]
            for j in range(group):
                total += jnp.where(owner == j, product[j * blocks : (j + 1) * blocks], 0.0)
            acc[2 * h + c] = total
        return carry

    lax.fori_loop(0, steps, project, 0)

    rows = pieces.shape[1]
    split = blocks // rows
    for h in range(halves):
        a, b = acc[2 * h], acc[2 * h + 1]
        both = (a[:, :half] + b[:, half:], b[:, :half] - a[:, half:])
        for c in range(2):
            for q in range(split):
                pieces[(2 * h + c) * split + q] = both[c][q * rows : (q + 1) * rows]

    started = []

    def send(source, target, sems, where):
        copy = pltpu.make_async_remote_copy(
            src_ref=source, dst_ref=target, send_sem=sems[0], recv_sem=sems[1], device_id=where, device_id_type=MESH
        )
        copy.start()
        started.append(copy)
        return copy

    size = n_space // 2
    mine = s % 2 * size
    send(
        pieces.at[pl.ds(size - mine, size)], land, (send_1.at[0], recv_1.at[0]), (f, mate)
    ).wait_recv()
    pieces[pl.ds(mine, size)] = pieces[pl.ds(mine, size)] + land[...]

    def chain(step, edge, end, arriving, leaving, i):
        def copy(to):
            return pltpu.make_async_remote_copy(
                src_ref=leaving, dst_ref=arriving, send_sem=send_1.at[i], recv_sem=recv_1.at[i],
                device_id=(f, to), device_id_type=MESH,
            )

        @pl.when(z == edge)
        def _():
            arriving[...] = jnp.zeros_like(arriving)

        @pl.when(z != edge)
        def _():
            copy(s - step).wait_recv()

        @pl.when(z != end)
        def _():
            leaving[...] = arriving[...] + pieces[pl.ds(mine, size)]
            copy(s + step).start()

    def go_up():
        chain(2, 0, top, below, upward, 1)

    def go_down():
        chain(-2, top, 0, above, downward, 2)

    @pl.when(2 * z <= top)
    def _():
        go_up()
        go_down()

    @pl.when(2 * z > top)
    def _():
        go_down()
        go_up()

    own[...] = ((below[...] + pieces[pl.ds(mine, size)] + above[...]) * factor).astype(own.dtype)
    second = []
    for df in range(1, n_freq):
        second.append(
            send(
                own, every.at[pl.ds(mine, size), f], (send_2.at[df], recv_2.at[df]), (lax.rem(f + df, n_freq), s)
            )
        )
    for swap in order[ahead:]:
        for df in range(1, n_freq):
            swap(df).start()
    every[pl.ds(mine, size), f] = own[...]
    for copy in second:
        copy.wait_recv()
    block = every.at[pl.ds(mine, size)]
    send(block, block, (send_3.at[0], recv_3.at[0]), (f, mate)).wait_recv()

    coefs = []
    for c in range(2):
        lanes = []
        for g in range(n_freq):
            for h in range(halves):
                base = (2 * h + c) * split
                lanes.append(
                    jnp.concatenate([every[base + q, g].astype(jnp.float32) for q in range(split)], axis=0)
                )
        coefs.append(jnp.concatenate(lanes, axis=1))
    for g, pair in enumerate(lines_of(coefs, groups)):
        for c in range(2):
            line_ref[g, c] = pair[c]
    mask = spread_mask(left_ref.shape[2], modes)

    def fill(g, carry):
        for c in range(2):
            lines = line_ref[g, c]
            for b in range(blocks):
                left_ref[g, (2 * b + c) * PAIR : (2 * b + c + 1) * PAIR] = jnp.where(
                    mask, lines[b : b + 1], 0.0
                ).astype(jnp.bfloat16)
        return carry

    lax.fori_loop(0, groups, fill, 0)

    half_length = length // 2

    def put_at(column, wide):
        def put(b, rows):
            early_ref[b * half_length : (b + 1) * half_length, pl.ds(column, wide)] = rows

        return put

    def finish(j, carry):
        for c in range(2):
            keep_broad(j, c).wait()
            for r in range(2):
                for df in range(1, n_freq):
                    swap_broad(j, c, r, df).wait_recv()
            broad[j, c, length] = broad[j, c, length // 2]
        synthesize(
            lambda g: stack_modes(broad, j, g, length), left_ref, basis_ref, mid_ref, 2 * tile,
            put_at(pl.multiple_of(j * 2 * tile, 2 * tile), 2 * tile),
        )
        return carry

    def arrived(j):
        for c in range(2):
            keep_narrow(j, c).wait()
            for df in range(1, n_freq):
                swap_narrow(j, c, df).wait_recv()
            narrow[j, c, length] = narrow[j, c, length // 2]

    if wides:
        lax.fori_loop(0, wides, finish, 0)
    last = narrows - 1
    for j in range(last):
        arrived(j)
        synthesize(
            lambda g: stack_modes(narrow, j, g, length), left_ref, basis_ref, mid_ref, tile,
            put_at((2 * wides + j) * tile, tile),
        )
    arrived(last)

    def arrange(g, carry):
        late_ref[g] = stack_modes(narrow, last, g, length)
        return carry

    lax.fori_loop(0, groups, arrange, 0)

    @pl.when(z < top)
    def _():
        pltpu.make_async_remote_copy(
            src_ref=upward, dst_ref=below, send_sem=send_1.at[1], recv_sem=recv_1.at[1],
            device_id=(f, s + 2), device_id_type=MESH,
        ).wait_send()

    @pl.when(z > 0)
    def _():
        pltpu.make_async_remote_copy(
            src_ref=downward, dst_ref=above, send_sem=send_1.at[2], recv_sem=recv_1.at[2],
            device_id=(f, s - 2), device_id_type=MESH,
        ).wait_send()

    for copy in started:
        copy.wait_send()
    for swap in order:
        for df in range(1, n_freq):
            swap(df).wait_send()


def gather(spectra, eigvecs, weights, basis, n_freq, n_space, blocks, factor, tile):
    _, count, modes, points = eigvecs.shape
    length = n_freq * count
    group = min(2 * PAIR, count)
    half = group * modes
    halves = count // group
    width = points // n_freq
    wides, narrows = width // (2 * tile) - 1, 2
    parts = 4
    cut = points // parts
    groups = length // (2 * PAIR)
    depth = 4 * PAIR * modes
    rows = halves * 2 * blocks // n_space
    out_rows = (blocks + 1) * (length // 2)
    hbm = pl.BlockSpec(memory_space=pltpu.HBM)
    vmem = pl.BlockSpec(memory_space=pltpu.VMEM)
    out_shape = [
        jax.ShapeDtypeStruct((out_rows, width - tile), jnp.float32),
        jax.ShapeDtypeStruct((groups, depth, tile), jnp.bfloat16),
        jax.ShapeDtypeStruct((groups, blocks * 2 * PAIR, depth), jnp.bfloat16),
    ]
    dma = pltpu.SemaphoreType.DMA
    return pl.pallas_call(
        functools.partial(gather_kernel, n_freq, n_space, group, parts, factor, wides),
        out_shape=out_shape,
        in_specs=[hbm] * 4,
        out_specs=[vmem] * len(out_shape),
        scratch_shapes=[
            pltpu.VMEM((max(wides, 1), 2, length + 1, modes, 2 * tile), jnp.bfloat16),
            pltpu.VMEM((narrows, 2, length + 1, modes, tile), jnp.bfloat16),
            pltpu.VMEM((2, 2, group * blocks, cut), jnp.bfloat16),
            pltpu.VMEM((2, 2, group, modes, cut), jnp.bfloat16),
            pltpu.VMEM((points,), jnp.bfloat16),
            pltpu.VMEM((parts, 1, cut), jnp.float32),
            pltpu.VMEM((2 * halves, blocks, 2 * half), jnp.float32),
            pltpu.VMEM((n_space, rows, half), jnp.float32),
            pltpu.VMEM((n_space // 2, rows, half), jnp.float32),
            pltpu.VMEM((n_space // 2, rows, half), jnp.float32),
            pltpu.VMEM((n_space // 2, rows, half), jnp.float32),
            pltpu.VMEM((n_space // 2, rows, half), jnp.float32),
            pltpu.VMEM((n_space // 2, rows, half), jnp.float32),
            pltpu.VMEM((n_space // 2, rows, half), jnp.bfloat16),
            pltpu.VMEM((n_space, n_freq, rows, half), jnp.bfloat16),
            pltpu.VMEM((groups, 2, blocks, depth), jnp.float32),
            pltpu.VMEM((blocks, length, 2 * tile), jnp.bfloat16),
            pltpu.VMEM((length, length), jnp.bfloat16),
            dma((max(wides, 1), 2, 2, n_freq)),
            dma((max(wides, 1), 2, 2, n_freq)),
            dma((narrows, 2, n_freq)),
            dma((narrows, 2, n_freq)),
            dma((max(wides, 1), 2)),
            dma((narrows, 2)),
            dma((2,)),
            dma((2,)),
            dma((2,)),
            dma((3,)),
            dma((3,)),
            dma((n_freq,)),
            dma((n_freq,)),
            dma((1,)),
            dma((1,)),
        ],
        compiler_params=pltpu.CompilerParams(
            collective_id=0, has_side_effects=True, vmem_limit_bytes=32 << 20
        ),
        cost_estimate=pl.CostEstimate(
            flops=8 * spectra.shape[1] * points * 2 * half, bytes_accessed=4 * spectra.size, transcendentals=0
        ),
        name="gather",
    )(*[pltpu.with_memory_space_constraint(x, pltpu.HBM) for x in (spectra, eigvecs, weights, basis)])


def finish_kernel(early_ref, late_ref, left_ref, basis_ref, out_ref, mid_ref, result, early_sem, late_sem):
    blocks, length, tile = mid_ref.shape
    half_length = length // 2
    rest = early_ref.shape[1]
    runs = late_sem.shape[0]
    copies = [pltpu.make_async_copy(early_ref, out_ref.at[:, :rest], early_sem)]
    copies[0].start()

    def put(b, rows):
        result[b * half_length : (b + 1) * half_length] = rows
        count = b + 1 if b < blocks - 1 else b
        if b != blocks - 1 and count % (blocks // runs) == 0:
            run = count // (blocks // runs) - 1
            start = run * (blocks // runs) * half_length
            span = slice(start, (b + 1) * half_length)
            copies.append(
                pltpu.make_async_copy(result.at[span], out_ref.at[span, rest : rest + tile], late_sem.at[run])
            )
            copies[-1].start()

    synthesize(lambda g: late_ref[g], left_ref, basis_ref, mid_ref, tile, put)
    wait_all(copies)


def finish(arrays, basis, blocks, length, width, tile):
    out_rows = (blocks + 1) * (length // 2)
    vmem = pl.BlockSpec(memory_space=pltpu.VMEM)
    runs = 4
    return pl.pallas_call(
        finish_kernel,
        out_shape=jax.ShapeDtypeStruct((out_rows, width), jnp.float32),
        in_specs=[vmem] * (len(arrays) + 1),
        out_specs=pl.BlockSpec(memory_space=pltpu.HBM),
        scratch_shapes=[
            pltpu.VMEM((blocks, length, tile), jnp.bfloat16),
            pltpu.VMEM((out_rows, tile), jnp.float32),
            pltpu.SemaphoreType.DMA,
            pltpu.SemaphoreType.DMA((runs,)),
        ],
        compiler_params=pltpu.CompilerParams(vmem_limit_bytes=24 << 20),
        cost_estimate=pl.CostEstimate(
            flops=4 * length * length * blocks * tile, bytes_accessed=4 * out_rows * width, transcendentals=0
        ),
        name="finish",
    )(*arrays, basis)


def basis_of(length):
    groups = length // (2 * PAIR)
    freq = np.arange(length // 2).reshape(groups, 1, PAIR)
    time = np.arange(length).reshape(length, 1, 1, 1)
    phase = 2.0 * np.pi * ((freq * time) % length) / length
    both = np.concatenate([np.cos(phase), -np.sin(phase)], axis=2)
    both[:, 0, 1, 0] = 1.0 - 2.0 * (np.arange(length) % 2)
    window = np.sin(np.pi * (np.arange(length) + 0.5) / length) / math.sqrt(length)
    return jnp.asarray((both.reshape(length, length) * window[:, None]).astype(np.float32)).astype(jnp.bfloat16)


def body(spectra, eigvecs, weights):
    n_freq = lax.axis_size("freq")
    n_space = lax.axis_size("space")
    _, count, blocks, points = spectra.shape
    factor = 1.0 / math.sqrt(points * n_space)
    length = n_freq * count
    width = points // n_freq
    tile = 128
    basis = basis_of(length)
    spectra = spectra.reshape(2, count * blocks, points)
    arrays = gather(spectra, eigvecs, weights, basis, n_freq, n_space, blocks, factor, tile)
    return finish(arrays, basis, blocks, length, width, tile)


def solution(mesh):
    placed = (P(None, "freq", None, "space"), P(None, "freq", None, "space"), P("space"))
    return jax.shard_map(
        body, mesh=mesh, in_specs=placed, out_specs=P(None, ("space", "freq")), check_vma=False
    )
```
